32 devices in a mesh: patch: 32 (over z, y, x, core).
Axes of the slice: x: 2, y: 2, z: 4, core: 2. Of those that a mesh axis runs over, the one named last changes fastest.
Arguments:
- grid_latent: bfloat16 [131072, 512], P('patch'), may hold values from -6 to 6
- mesh_latent: bfloat16 [10240, 512], P('patch'), may hold values from -6 to 6
- mesh_cotangent: bfloat16 [10240, 512], P('patch'), may hold values from -6 to 6
- grid_rows: int32 [12288], P('patch'), may hold values from 0 to 4095
- mesh_rows: int32 [12288], P('patch'), may hold values from 0 to 319
- counts: int32 [32, 32], P('patch'), may hold values from 1 to 12, as said below
- w1_grid: bfloat16 [512, 512], replicated, may hold values from -0.25 to 0.25
- w1_mesh: bfloat16 [512, 512], replicated, may hold values from -0.25 to 0.25
- bias_one: float32 [512], replicated, may hold values from -3 to 3
- w2: bfloat16 [512, 512], replicated, may hold values from -0.25 to 0.25
Outputs:
- grid_grad: float32 [131072, 512], P('patch')
- mesh_grad: float32 [10240, 512], P('patch')
- w1_grid_grad: float32 [512, 512], replicated
- w1_mesh_grad: float32 [512, 512], replicated
- w2_grad: float32 [512, 512], replicated
- bias_grad: float32 [512], replicated
The draws below stay inside these ranges and needn't reach their ends.
Inputs may be any that keep to these rules, and one draw needn't show every extreme that they name: counts[p, q] of the 12 slots from patch p to owner q are live, the first ones; every row and every column of counts has at least one entry equal to 12. `grid_rows`: padding slots hold arbitrary rows in range.
All inputs are finite; a program needn't handle non-finite values.
Results may differ from the reference program's by a relative error of at most 0.007.
Values may be sent and summed in bfloat16 or wider, within the bound.
No kernel may reach another device: no remote copies, remote signals or barrier semaphores. Data moves between devices by JAX's collectives and lax.ppermute only.
A program may use at most 128 MiB of HBM per device.

```python
import jax
import jax.numpy as jnp
from jax import lax

D = 512
MLP_W = 512
C = 12
G_DEV = 4096
M_DEV = 320
SLOTS = 12288
GRID = 131072
MESH = 10240
N_PATCH = 32


def draw_counts(key, part):
    base_key = jax.random.fold_in(key, 7)
    key_base, key_level, key_pairs = jax.random.split(base_key, 3)
    base_load = jax.random.randint(key_base, (N_PATCH, N_PATCH), C // 2, C + 1)
    load_level = jax.random.randint(key_level, (N_PATCH, 1), 2, 5)
    loaded = jnp.maximum(1, base_load * load_level // 4)
    shuffled = jax.random.permutation(key_pairs, N_PATCH)
    full_pair = jnp.arange(N_PATCH)[None, :] == shuffled[:, None]
    return jnp.where(full_pair, C, loaded).astype(jnp.int32)


def place_ends(result, key, least, largest):
    index_at = [jax.random.randint(jax.random.fold_in(key, axis), (), 0, length) for axis, length in enumerate(result.shape)]
    widest = result.shape.index(max(result.shape))
    beside = index_at[:widest] + [(index_at[widest] + 1) % result.shape[widest]] + index_at[widest + 1:]
    return result.at[tuple(index_at)].set(least).at[tuple(beside)].set(largest)


def level_of(stream_key, extent, cuts, smallest, high):
    def one(dim, parts):
        heights = jax.random.uniform(jax.random.fold_in(jax.random.fold_in(stream_key, 6), dim), (parts,), jnp.float32, smallest / len(cuts), high / len(cuts))
        return jnp.repeat(jnp.exp(heights), extent[dim] // parts).reshape((-1,) + (1,) * (len(extent) - dim - 1))

    loudness = one(*cuts[0])
    for cut in cuts[1:]:
        loudness = loudness * one(*cut)
    return loudness


def scatter_about(key, extent, spread, reach, cuts=(), held_as=jnp.bfloat16):
    values = spread * jax.random.normal(key, extent, jnp.float32)
    if cuts:
        values = values * level_of(key, extent, cuts, -0.22, 0.18)
    return jnp.clip(values, -reach, reach).astype(held_as)


def setup_inputs(seed: int = 0) -> dict:
    seeds = jax.random.split(jax.random.key(seed), 11)
    grid_latent = scatter_about(seeds[0], (GRID, D), 1.0, 6.0, ((0, 32),))
    mesh_latent = scatter_about(seeds[1], (MESH, D), 1.0, 6.0, ((0, 32),))
    mesh_cotangent = scatter_about(seeds[2], (MESH, D), 1.0, 6.0, ((0, 32),))
    grid_rows = place_ends(jax.random.randint(seeds[3], (SLOTS,), 0, G_DEV), jax.random.fold_in(seeds[3], 1), 0, G_DEV - 1).astype(jnp.int32)
    mesh_rows = place_ends(jax.random.randint(seeds[4], (SLOTS,), 0, M_DEV), jax.random.fold_in(seeds[4], 1), 0, M_DEV - 1).astype(jnp.int32)
    counts = draw_counts(jax.random.fold_in(seeds[10], 71), 0)
    w1_grid = scatter_about(seeds[6], (D, MLP_W), D ** -0.5, 0.25)
    w1_mesh = scatter_about(seeds[7], (D, MLP_W), D ** -0.5, 0.25)
    bias_one = scatter_about(seeds[8], (MLP_W,), 0.5, 3.0, (), jnp.float32)
    w2 = scatter_about(seeds[9], (MLP_W, D), MLP_W ** -0.5, 0.25)
    return {"grid_latent": grid_latent, "mesh_latent": mesh_latent, "mesh_cotangent": mesh_cotangent, "grid_rows": grid_rows, "mesh_rows": mesh_rows, "counts": counts, "w1_grid": w1_grid, "w1_mesh": w1_mesh, "bias_one": bias_one, "w2": w2}


def reference(grid_latent, mesh_latent, mesh_cotangent, grid_rows, mesh_rows, counts, w1_grid, w1_mesh, bias_one, w2):
    per_patch = N_PATCH * C
    slot_ids = jnp.arange(per_patch, dtype=jnp.int32)
    owners = slot_ids // C
    within = slot_ids % C
    grid_local = grid_rows.reshape(N_PATCH, per_patch)
    mesh_local = mesh_rows.reshape(N_PATCH, per_patch)
    senders = jnp.arange(N_PATCH, dtype=jnp.int32)

    def accumulate(carried, inputs):
        grid_acc, wg_acc, wm_acc, w2_acc, bias_acc = carried
        sender, grid_part, mesh_part, sent_counts = inputs
        grid_index = (owners * G_DEV + grid_part).astype(jnp.int32)
        mesh_index = (sender * M_DEV + mesh_part).astype(jnp.int32)
        live_mask = within < sent_counts[owners]
        grid_in = grid_latent[grid_index]
        mesh_in = mesh_latent[mesh_index]
        grid_proj = jnp.dot(grid_in, w1_grid, preferred_element_type=jnp.float32).astype(jnp.bfloat16)
        before = grid_proj.astype(jnp.float32) + jnp.dot(mesh_in, w1_mesh, preferred_element_type=jnp.float32) + bias_one
        logistic = jax.nn.sigmoid(before)
        hidden = (before * logistic).astype(jnp.bfloat16)
        derivative = logistic * (1.0 + before * (1.0 - logistic))
        out_grad = jnp.where(live_mask[:, None], mesh_cotangent[mesh_index], jnp.zeros((), jnp.bfloat16))
        hid_grad = jnp.dot(out_grad, w2.T, preferred_element_type=jnp.float32)
        pre_grad = (hid_grad * derivative).astype(jnp.bfloat16)
        edge_grid = jnp.dot(pre_grad, w1_grid.T, preferred_element_type=jnp.float32).astype(jnp.bfloat16)
        grid_acc = grid_acc.at[grid_index].add(edge_grid.astype(jnp.float32))
        node_sum = jax.ops.segment_sum(pre_grad.astype(jnp.float32), mesh_part, num_segments=M_DEV)
        mesh_block = jnp.dot(node_sum, w1_mesh.T.astype(jnp.float32), precision=lax.Precision.HIGHEST)
        wg_acc = wg_acc + jnp.dot(grid_in.T, pre_grad, preferred_element_type=jnp.float32)
        wm_acc = wm_acc + jnp.dot(mesh_in.T, pre_grad, preferred_element_type=jnp.float32)
        w2_acc = w2_acc + jnp.dot(hidden.T, out_grad, preferred_element_type=jnp.float32)
        bias_acc = bias_acc + lax.optimization_barrier(jnp.sum(pre_grad.astype(jnp.float32), axis=0))
        return ((grid_acc, wg_acc, wm_acc, w2_acc, bias_acc), mesh_block)
    start = (jnp.zeros((G_DEV * N_PATCH, D), jnp.float32), jnp.zeros((D, MLP_W), jnp.float32), jnp.zeros((D, MLP_W), jnp.float32), jnp.zeros((MLP_W, D), jnp.float32), jnp.zeros((MLP_W,), jnp.float32))
    finals, mesh_blocks = lax.scan(accumulate, start, (senders, grid_local, mesh_local, counts))
    grid_grad, wg_acc, wm_acc, w2_acc, bias_acc = finals
    norm_scale = 1.0 / jnp.sqrt(jnp.float32(N_PATCH * N_PATCH * C))
    mesh_grad = mesh_blocks.reshape(N_PATCH * M_DEV, D)
    return (grid_grad, mesh_grad, wg_acc * norm_scale, wm_acc * norm_scale, w2_acc * norm_scale, bias_acc * norm_scale)
```

```python
import functools
import math

import jax
import jax.numpy as jnp
from jax import lax
from jax.experimental import pallas as pl
from jax.experimental.pallas import tpu as pltpu
from jax.sharding import PartitionSpec as P

SUB = 8
HALF = SUB // 2
F32 = jnp.float32
BF16 = jnp.bfloat16
WHOLE = pl.BlockSpec(memory_space=pltpu.VMEM)
GRANT = pltpu.CompilerParams(vmem_limit_bytes=24 << 20)


def dot(left, right, dims=((1,), (0,))):
    return lax.dot_general(left, right, (dims, ((), ())), preferred_element_type=F32)


def near(value):
    return pltpu.with_memory_space_constraint(value, pltpu.VMEM)


def call(kernel, outs, scratch=(), flops=0, leaves=False):
    make = jax.ShapeDtypeStruct if leaves else pltpu.VMEM
    built = pl.pallas_call(
        kernel,
        out_shape=[make(shape, dtype) for shape, dtype in outs],
        scratch_shapes=list(scratch),
        compiler_params=GRANT,
        cost_estimate=pl.CostEstimate(flops=flops, transcendentals=0, bytes_accessed=0),
    )
    return lambda *values: built(*map(near, values))


def column(index):
    members, capacity = index.shape
    middle = members // 2
    lane = lax.broadcasted_iota(jnp.int32, (members, SUB, capacity), 2)
    row = lax.broadcasted_iota(jnp.int32, (members, SUB, capacity), 1)
    spread = jnp.broadcast_to(index[:, None, :], (members, SUB, capacity))
    head = jnp.sum(jnp.where(lane == row, spread, 0).astype(F32), axis=2, keepdims=True)
    upper = row[:middle] < HALF
    chosen = jnp.where(upper, spread[:middle], spread[middle:])
    wanted = jnp.where(upper, row[:middle] + SUB, row[:middle] + HALF)
    tail = jnp.sum(jnp.where(lane[:middle] == wanted, chosen, 0).astype(F32), axis=2, keepdims=True)
    return jnp.concatenate(
        (head.reshape(members * SUB, 1), tail.reshape(middle * SUB, 1)), axis=0
    ).astype(jnp.int32)


def lanes(index):
    col = column(index).astype(F32)
    return jnp.transpose(jnp.broadcast_to(col, (col.shape[0], 128)))[:1].astype(jnp.int32)


def pick(col, start, size):
    at = lax.broadcasted_iota(jnp.int32, (col.shape[0], size), 1) + start
    return jnp.where(at == col, 1.0, 0.0).astype(BF16)


def pack(rows, members):
    width = rows.shape[1]
    middle = members // 2
    head = rows[: members * SUB].reshape(members, SUB, width)
    tail = rows[members * SUB :].reshape(middle, SUB, width)
    left, right = tail[:, :, : width // 2], tail[:, :, width // 2 :]
    upper = lax.broadcasted_iota(jnp.int32, left.shape, 1) < HALF
    first = jnp.where(upper, left, pltpu.roll(right, HALF, 1))
    second = jnp.where(upper, pltpu.roll(left, HALF, 1), right)
    return head, jnp.concatenate((first, second), axis=0)


def unpack(packed, width):
    members = packed.shape[0]
    middle = members // 2
    head = packed[:, :, :width].reshape(members * SUB, width)
    first = packed[:middle, :, width : width + width // 2]
    second = packed[middle:, :, width : width + width // 2]
    upper = lax.broadcasted_iota(jnp.int32, first.shape, 1) < HALF
    left = jnp.where(upper, first, pltpu.roll(second, HALF, 1))
    right = jnp.where(upper, pltpu.roll(first, HALF, 1), second)
    tail = jnp.concatenate((left, right), axis=2).reshape(middle * SUB, width)
    return jnp.concatenate((head, tail), axis=0)


def gather_kernel(index_ref, table_ref, out_ref):
    members = index_ref.shape[0]
    width = table_ref.shape[1]
    col = column(index_ref[...])
    step = min(512, table_ref.shape[0])
    total = None
    for start in range(0, table_ref.shape[0], step):
        part = dot(pick(col, start, step), table_ref[start : start + step, :])
        total = part if total is None else total + part
    head, tail = pack(total, members)
    out_ref[:, :, :width] = head.astype(BF16)
    out_ref[:, :, width:] = tail.astype(BF16)


def mesh_kernel(
    rows_ref, live_ref, latent_ref, cot_ref, w1_ref, w2_ref, bias_ref, in_ref, grad_ref, base_ref, hid_ref
):
    nodes = latent_ref.shape[0]
    mesh_in = dot(pick(column(rows_ref[...]), 0, nodes), latent_ref[...]).astype(BF16)
    out_grad = dot(pick(column(live_ref[...]), 0, nodes), cot_ref[...]).astype(BF16)
    in_ref[...] = mesh_in
    grad_ref[...] = out_grad
    base_ref[...] = dot(mesh_in, w1_ref[...]) + bias_ref[...]
    hid_ref[...] = dot(out_grad, w2_ref[...], ((1,), (1,)))


def edge_kernel(
    got_ref, base_ref, hid_ref, mesh_ref, grad_ref, w1_ref, sent_ref, kept_ref, pre_ref, full_ref
):
    width = mesh_ref.shape[1]
    half = sent_ref.shape[1]
    core = lax.rem(lax.axis_index("patch"), 2)
    grid_in = unpack(got_ref[...].astype(F32), width).astype(BF16)
    before = dot(grid_in, w1_ref[...]).astype(BF16).astype(F32) + base_ref[...]
    logistic = jax.nn.sigmoid(before)
    hidden = (before * logistic).astype(BF16)
    derivative = logistic * (1.0 + before * (1.0 - logistic))
    pre = (hid_ref[...] * derivative).astype(BF16)
    pre_ref[...] = pre
    across = ((0,), (0,))
    full_ref[0] = dot(grid_in, pre, across)
    full_ref[1] = dot(mesh_ref[...], pre, across)
    full_ref[2] = dot(hidden, grad_ref[...], across)
    for which in range(3):
        away = pl.multiple_of((1 - core) * half, half)
        home = pl.multiple_of(core * half, half)
        sent_ref[which] = full_ref[which, pl.ds(away, half), :].astype(BF16)
        kept_ref[which] = full_ref[which, pl.ds(home, half), :]


def return_kernel(pre_ref, w1_ref, out_ref):
    members = out_ref.shape[0]
    width = pre_ref.shape[1]
    pre = pre_ref[...]
    head, tail = pack(dot(pre, w1_ref[...], ((1,), (1,))), members)
    out_ref[:, :, :width] = head.astype(BF16)
    out_ref[:, :, width : width + width // 2] = tail.astype(BF16)
    bias = jnp.sum(pre.astype(F32), axis=0, keepdims=True)
    high = bias.astype(BF16).astype(F32)
    low = bias - high
    at = lax.broadcasted_iota(jnp.int32, (SUB, 128), 0)
    tile = jnp.zeros((SUB, 128), F32)
    for part in range(width // 128):
        block = slice(part * 128, part * 128 + 128)
        tile = jnp.where(at == part, high[:, block], tile)
        tile = jnp.where(at == part + width // 128, low[:, block], tile)
    out_ref[:, :, width + width // 2 :] = jnp.broadcast_to(tile[None], (members, SUB, 128)).astype(
        BF16
    )


def scatter_kernel(index_ref, came_ref, out_ref, rows_ref, flat_ref):
    step = pl.program_id(0)
    size, width = out_ref.shape

    @pl.when(step == 0)
    def _():
        flat_ref[...] = jnp.broadcast_to(lanes(index_ref[...]), flat_ref.shape)
        rows_ref[...] = unpack(came_ref[...].astype(F32), width).astype(BF16)

    at = lax.broadcasted_iota(jnp.int32, (size, rows_ref.shape[0]), 0) + step * size
    chosen = jnp.where(at == flat_ref[:1], 1.0, 0.0).astype(BF16)
    out_ref[...] = dot(chosen, rows_ref[...])


def bias_kernel(scale, came_ref, out_ref):
    width = out_ref.shape[1]
    tile = jnp.sum(came_ref[:, :, width + width // 2 :].astype(F32), axis=0)
    for part in range(width // 128):
        low = part + width // 128
        out_ref[:, part * 128 : part * 128 + 128] = (
            tile[part : part + 1] + tile[low : low + 1]
        ) * scale


def node_kernel(rows_ref, pre_ref, w1_ref, out_ref):
    nodes = out_ref.shape[0]
    flat = lanes(rows_ref[...])
    at = lax.broadcasted_iota(jnp.int32, (nodes, flat.shape[1]), 0)
    sums = dot(jnp.where(at == flat, 1.0, 0.0).astype(BF16), pre_ref[...])
    total = None
    for _ in range(3):
        piece = sums.astype(BF16)
        part = dot(piece, w1_ref[...], ((1,), (1,)))
        total = part if total is None else total + part
        sums = sums - piece.astype(F32)
    out_ref[...] = total


def place(stride, size):
    return lax.rem(lax.div(lax.axis_index("patch"), stride), size)


def fold(own, came, stride, size):
    count, rows, width = own.shape
    cut = rows // size

    def kernel(*refs):
        inputs, outputs = refs[: 1 + len(came)], refs[1 + len(came) :]
        here = place(stride, size) if size > 1 else 0
        for k, out_ref in enumerate(outputs):
            start = pl.multiple_of((here ^ k) * cut, cut) if size > 1 else 0
            total = sum(ref[:, pl.ds(start, cut), :].astype(F32) for ref in inputs)
            out_ref[...] = total.astype(out_ref.dtype)

    types = [F32 if k == 0 and size > 1 else BF16 for k in range(size)]
    if cut % 16 == 0:
        return call(kernel, [((count, cut, width), dtype) for dtype in types])(own, *came)
    total = own.astype(F32) + sum(part.astype(F32) for part in came)
    here = place(stride, size) if size > 1 else 0
    return [
        lax.dynamic_slice_in_dim(total, (here ^ k) * cut, cut, axis=1).astype(dtype)
        for k, dtype in enumerate(types)
    ]


def join(pieces, stride):
    count, cut, width = pieces[0].shape
    size = len(pieces)

    def kernel(*refs):
        here = place(stride, size)
        for k in range(size):
            start = pl.multiple_of((here ^ k) * cut, cut)
            refs[-1][:, pl.ds(start, cut), :] = refs[k][...]

    if cut % 16 == 0:
        return call(kernel, [((count, cut * size, width), BF16)])(*pieces)[0]
    order = jnp.arange(size, dtype=jnp.int32) ^ place(stride, size)
    return jnp.take(jnp.stack(pieces, axis=1), order, axis=1).reshape(count, cut * size, width)


def send(value, step, members):
    return lax.ppermute(value, "patch", [(i, i ^ step) for i in range(members)])


def final_kernel(scale, stride, size, *refs):
    pieces, outputs = refs[: 2 * size], refs[2 * size :]
    core = lax.rem(lax.axis_index("patch"), 2)
    here = place(stride, size)
    cut = pieces[0].shape[1]
    for side in range(2):
        base = (core if side == 0 else 1 - core) * (cut * size)
        for k in range(size):
            start = pl.multiple_of(base + (here ^ k) * cut, cut)
            for which, out_ref in enumerate(outputs):
                out_ref[pl.ds(start, cut), :] = pieces[side * size + k][which].astype(F32) * scale


def body(
    grid_latent,
    mesh_latent,
    mesh_cotangent,
    grid_rows,
    mesh_rows,
    counts,
    w1_grid,
    w1_mesh,
    bias_one,
    w2,
):
    members = lax.axis_size("patch")
    slots = grid_rows.shape[0]
    capacity = slots // members
    width = grid_latent.shape[1]
    nodes = mesh_latent.shape[0]
    points = grid_latent.shape[0]
    if capacity != SUB + HALF or members & (members - 1):
        raise ValueError("slot layout")
    scale = 1.0 / math.sqrt(members * slots)
    steps = []
    rest, stride = members // 2, 2
    while rest > 1:
        size = 4 if rest % 4 == 0 else 2
        steps.append((stride, size))
        rest, stride = rest // size, stride * size

    swap = functools.partial(
        lax.all_to_all, axis_name="patch", split_axis=0, concat_axis=0, tiled=True
    )
    wanted = swap(grid_rows.reshape(members, capacity))
    rows2d = mesh_rows.reshape(members, capacity)
    slot = jnp.arange(capacity, dtype=jnp.int32)[None, :]
    live2d = jnp.where(slot < counts[0][:, None], rows2d, -1)
    packed = (members, SUB, width + width // 2)
    found = call(gather_kernel, [(packed, BF16)], flops=2 * slots * points * width)(
        wanted, grid_latent
    )[0]
    got = swap(found)
    flat = (slots, width)
    mesh_in, out_grad, base, hid = call(
        mesh_kernel, [(flat, BF16), (flat, BF16), (flat, F32), (flat, F32)], flops=8 * slots * width**2
    )(rows2d, live2d, mesh_latent, mesh_cotangent, w1_mesh, w2, bias_one.reshape(1, width))
    halves = (3, width // 2, width)
    sent, kept, pre = call(
        edge_kernel,
        [(halves, BF16), (halves, F32), (flat, BF16)],
        [pltpu.VMEM((3, width, width), F32)],
        flops=8 * slots * width**2,
    )(got, base, hid, mesh_in, out_grad, w1_grid)

    came = [send(sent, 1, members)]
    own = kept
    for stride, size in steps:
        own, *away = fold(own, came, stride, size)
        came = [send(part, k * stride, members) for k, part in enumerate(away, 1)]
    pieces = [fold(own, came, 1, 1)[0]]
    for position, (stride, size) in reversed(list(enumerate(steps))):
        share = pieces[0]
        pieces = [share] + [send(share, k * stride, members) for k in range(1, size)]
        if position > 0:
            pieces = [join(pieces, stride)]
    stride, size = steps[0]
    others = [send(piece, 1, members) for piece in pieces]
    grads = call(
        functools.partial(final_kernel, scale, stride, size), [((width, width), F32)] * 3, leaves=True
    )(*pieces, *others)

    leaving = call(
        return_kernel, [((members, SUB, 2 * width - width // 2 + 128), BF16)], flops=2 * slots * width**2
    )(pre, w1_grid)[0]
    returned = swap(leaving)
    block = min(512, points)
    grid_grad = pl.pallas_call(
        scatter_kernel,
        out_shape=jax.ShapeDtypeStruct((points, width), F32),
        grid=(points // block,),
        compiler_params=GRANT,
        in_specs=[WHOLE, WHOLE],
        out_specs=pl.BlockSpec((block, width), lambda i: (i, 0)),
        scratch_shapes=[pltpu.VMEM(flat, BF16), pltpu.VMEM((SUB, slots), jnp.int32)],
        cost_estimate=pl.CostEstimate(
            flops=2 * slots * points * width, transcendentals=0, bytes_accessed=4 * points * width
        ),
    )(near(wanted), near(returned))
    bias_grad = call(functools.partial(bias_kernel, scale), [((1, width), F32)], leaves=True)(returned)[0]
    mesh_grad = call(node_kernel, [((nodes, width), F32)], flops=8 * nodes * width**2, leaves=True)(
        rows2d, pre, w1_mesh
    )[0]
    return (grid_grad, mesh_grad, *grads, bias_grad.reshape(width))


def solution(mesh):
    rows, line = P("patch", None), P("patch")
    return jax.shard_map(
        body,
        mesh=mesh,
        in_specs=(rows, rows, rows, line, line, rows, P(), P(), P(), P()),
        out_specs=(rows, rows, P(), P(), P(), P()),
        check_vma=False,
    )
```

```python
import functools
import math

import jax
import jax.numpy as jnp
from jax import lax
from jax.experimental import pallas as pl
from jax.experimental.pallas import tpu as pltpu
from jax.sharding import PartitionSpec as P


SUB = 8
HALF = SUB // 2
F32 = jnp.float32
BF16 = jnp.bfloat16
WHOLE = pl.BlockSpec(memory_space=pltpu.VMEM)
FAR = pl.BlockSpec(memory_space=pltpu.HBM)
GRANT = pltpu.CompilerParams(vmem_limit_bytes=30 << 20)


def dot(left, right, dims=((1,), (0,))):
    return lax.dot_general(left, right, (dims, ((), ())), preferred_element_type=F32)


def near(value):
    return pltpu.with_memory_space_constraint(value, pltpu.VMEM)


def far(value):
    return pltpu.with_memory_space_constraint(value, pltpu.HBM)


def call(kernel, outs, scratch=(), flops=0, leaves=False, specs=None):
    make = jax.ShapeDtypeStruct if leaves else pltpu.VMEM
    built = pl.pallas_call(
        kernel,
        **({} if specs is None else {"in_specs": specs}),
        out_shape=[make(shape, dtype) for shape, dtype in outs],
        scratch_shapes=list(scratch),
        compiler_params=GRANT,
        cost_estimate=pl.CostEstimate(flops=flops, transcendentals=0, bytes_accessed=0),
    )
    places = [near] * 99 if specs is None else [far if spec is FAR else near for spec in specs]
    return lambda *values: built(*(place(value) for place, value in zip(places, values)))


def column(index):
    members, capacity = index.shape
    middle = members // 2
    lane = lax.broadcasted_iota(jnp.int32, (members, SUB, capacity), 2)
    row = lax.broadcasted_iota(jnp.int32, (members, SUB, capacity), 1)
    spread = jnp.broadcast_to(index[:, None, :], (members, SUB, capacity))
    head = jnp.sum(jnp.where(lane == row, spread, 0).astype(F32), axis=2, keepdims=True)
    upper = row[:middle] < HALF
    chosen = jnp.where(upper, spread[:middle], spread[middle:])
    wanted = jnp.where(upper, row[:middle] + SUB, row[:middle] + HALF)
    tail = jnp.sum(jnp.where(lane[:middle] == wanted, chosen, 0).astype(F32), axis=2, keepdims=True)
    return jnp.concatenate(
        (head.reshape(members * SUB, 1), tail.reshape(middle * SUB, 1)), axis=0
    ).astype(jnp.int32)


def lanes(index):
    col = column(index).astype(F32)
    return jnp.transpose(jnp.broadcast_to(col, (col.shape[0], 128)))[:1].astype(jnp.int32)


def pick(col, start, size):
    at = lax.broadcasted_iota(jnp.int32, (col.shape[0], size), 1) + start
    return jnp.where(at == col, 1.0, 0.0).astype(BF16)


def pack(rows, members):
    width = rows.shape[1]
    middle = members // 2
    head = rows[: members * SUB].reshape(members, SUB, width)
    tail = rows[members * SUB :].reshape(middle, SUB, width)
    left, right = tail[:, :, : width // 2], tail[:, :, width // 2 :]
    upper = lax.broadcasted_iota(jnp.int32, left.shape, 1) < HALF
    first = jnp.where(upper, left, pltpu.roll(right, HALF, 1))
    second = jnp.where(upper, pltpu.roll(left, HALF, 1), right)
    return head, jnp.concatenate((first, second), axis=0)


def unpack(packed, width):
    members = packed.shape[0]
    middle = members // 2
    head = packed[:, :, :width].reshape(members * SUB, width)
    first = packed[:middle, :, width : width + width // 2]
    second = packed[middle:, :, width : width + width // 2]
    upper = lax.broadcasted_iota(jnp.int32, first.shape, 1) < HALF
    left = jnp.where(upper, first, pltpu.roll(second, HALF, 1))
    right = jnp.where(upper, pltpu.roll(first, HALF, 1), second)
    tail = jnp.concatenate((left, right), axis=2).reshape(middle * SUB, width)
    return jnp.concatenate((head, tail), axis=0)


def gather_kernel(index_ref, table_ref, out_ref, held_ref, sems):
    members = index_ref.shape[0]
    width = table_ref.shape[1]
    count, step, _ = held_ref.shape
    copies = [
        pltpu.make_async_copy(table_ref.at[pl.ds(k * step, step), :], held_ref.at[k], sems.at[k])
        for k in range(count)
    ]
    for copy in copies:
        copy.start()
    col = column(index_ref[...])
    total = None
    for k, copy in enumerate(copies):
        chosen = pick(col, k * step, step)
        copy.wait()
        part = dot(chosen, held_ref[k])
        total = part if total is None else total + part
    head, tail = pack(total, members)
    out_ref[:, :, :width] = head.astype(BF16)
    out_ref[:, :, width:] = tail.astype(BF16)


def edge_kernel(
    got_ref,
    rows_ref,
    live_ref,
    latent_ref,
    cot_ref,
    w1m_ref,
    w2_ref,
    bias_ref,
    w1g_ref,
    sent_ref,
    kept_ref,
    pre_ref,
    full_ref,
    latent_vmem,
    cot_vmem,
    sems,
):
    nodes, width = latent_ref.shape
    load_latent = pltpu.make_async_copy(latent_ref, latent_vmem, sems.at[0])
    load_cot = pltpu.make_async_copy(cot_ref, cot_vmem, sems.at[1])
    load_latent.start()
    load_cot.start()
    half = sent_ref.shape[1]
    core = lax.rem(lax.axis_index("patch"), 2)
    grid_in = unpack(got_ref[...].astype(F32), width).astype(BF16)
    grid_proj = dot(grid_in, w1g_ref[...]).astype(BF16).astype(F32)
    picked = pick(column(rows_ref[...]), 0, nodes)
    live = pick(column(live_ref[...]), 0, nodes)
    load_latent.wait()
    mesh_in = dot(picked, latent_vmem[...]).astype(BF16)
    load_cot.wait()
    out_grad = dot(live, cot_vmem[...]).astype(BF16)
    before = grid_proj + dot(mesh_in, w1m_ref[...]) + bias_ref[...]
    logistic = jax.nn.sigmoid(before)
    hidden = (before * logistic).astype(BF16)
    derivative = logistic * (1.0 + before * (1.0 - logistic))
    pre = (dot(out_grad, w2_ref[...], ((1,), (1,))) * derivative).astype(BF16)
    pre_ref[...] = pre
    across = ((0,), (0,))
    full_ref[0] = dot(grid_in, pre, across)
    full_ref[1] = dot(mesh_in, pre, across)
    full_ref[2] = dot(hidden, out_grad, across)
    away = pl.multiple_of((1 - core) * half, half)
    home = pl.multiple_of(core * half, half)
    for which in range(3):
        sent_ref[which] = full_ref[which, pl.ds(away, half), :].astype(BF16)
        kept_ref[which] = full_ref[which, pl.ds(home, half), :]


def return_kernel(pre_ref, w1_ref, after_ref, out_ref):
    members = out_ref.shape[0]
    width = pre_ref.shape[1]
    pre = pre_ref[...]
    head, tail = pack(dot(pre, w1_ref[...], ((1,), (1,))), members)
    out_ref[:, :, :width] = head.astype(BF16)
    out_ref[:, :, width : width + width // 2] = tail.astype(BF16)
    bias = jnp.sum(pre.astype(F32), axis=0, keepdims=True)
    high = bias.astype(BF16).astype(F32)
    low = bias - high
    at = lax.broadcasted_iota(jnp.int32, (SUB, 128), 0)
    tile = jnp.zeros((SUB, 128), F32)
    for part in range(width // 128):
        block = slice(part * 128, part * 128 + 128)
        tile = jnp.where(at == part, high[:, block], tile)
        tile = jnp.where(at == part + width // 128, low[:, block], tile)
    out_ref[:, :, width + width // 2 :] = jnp.broadcast_to(tile[None], (members, SUB, 128)).astype(
        BF16
    )


def scatter_kernel(index_ref, came_ref, after_ref, out_ref, rows_ref, flat_ref):
    step = pl.program_id(0)
    size, width = out_ref.shape

    @pl.when(step == 0)
    def _():
        flat_ref[...] = jnp.broadcast_to(lanes(index_ref[...]), flat_ref.shape)
        rows_ref[...] = unpack(came_ref[...].astype(F32), width).astype(BF16)

    at = lax.broadcasted_iota(jnp.int32, (size, rows_ref.shape[0]), 0) + step * size
    chosen = jnp.where(at == flat_ref[:1], 1.0, 0.0).astype(BF16)
    out_ref[...] = dot(chosen, rows_ref[...])


def bias_kernel(scale, came_ref, out_ref):
    width = out_ref.shape[1]
    tile = jnp.sum(came_ref[:, :, width + width // 2 :].astype(F32), axis=0)
    for part in range(width // 128):
        low = part + width // 128
        out_ref[:, part * 128 : part * 128 + 128] = (
            tile[part : part + 1] + tile[low : low + 1]
        ) * scale


def node_kernel(rows_ref, pre_ref, w1_ref, after_ref, out_ref):
    nodes = out_ref.shape[0]
    flat = lanes(rows_ref[...])
    at = lax.broadcasted_iota(jnp.int32, (nodes, flat.shape[1]), 0)
    sums = dot(jnp.where(at == flat, 1.0, 0.0).astype(BF16), pre_ref[...])
    total = None
    for _ in range(3):
        piece = sums.astype(BF16)
        part = dot(piece, w1_ref[...], ((1,), (1,)))
        total = part if total is None else total + part
        sums = sums - piece.astype(F32)
    out_ref[...] = total


def place(stride, size):
    return lax.rem(lax.div(lax.axis_index("patch"), stride), size)


def fold(own, came, stride, size):
    count, rows, width = own.shape
    cut = rows // size

    def kernel(*refs):
        inputs, outputs = refs[: 1 + len(came)], refs[1 + len(came) :]
        here = place(stride, size) if size > 1 else 0
        for k, out_ref in enumerate(outputs):
            start = pl.multiple_of((here ^ k) * cut, cut) if size > 1 else 0
            total = sum(ref[:, pl.ds(start, cut), :].astype(F32) for ref in inputs)
            out_ref[...] = total.astype(out_ref.dtype)

    types = [F32 if k == 0 and size > 1 else BF16 for k in range(size)]
    if cut % 16 == 0:
        return call(kernel, [((count, cut, width), dtype) for dtype in types])(own, *came)
    total = own.astype(F32) + sum(part.astype(F32) for part in came)
    here = place(stride, size) if size > 1 else 0
    return [
        lax.dynamic_slice_in_dim(total, (here ^ k) * cut, cut, axis=1).astype(dtype)
        for k, dtype in enumerate(types)
    ]


def join(pieces, stride):
    count, cut, width = pieces[0].shape
    size = len(pieces)

    def kernel(*refs):
        here = place(stride, size)
        for k in range(size):
            start = pl.multiple_of((here ^ k) * cut, cut)
            refs[-1][:, pl.ds(start, cut), :] = refs[k][...]

    if cut % 16 == 0:
        return call(kernel, [((count, cut * size, width), BF16)])(*pieces)[0]
    order = jnp.arange(size, dtype=jnp.int32) ^ place(stride, size)
    return jnp.take(jnp.stack(pieces, axis=1), order, axis=1).reshape(count, cut * size, width)


def send(value, step, members):
    return lax.ppermute(value, "patch", [(i, i ^ step) for i in range(members)])


def final_kernel(scale, stride, size, *refs):
    pieces, outputs = refs[: 2 * size], refs[2 * size :]
    core = lax.rem(lax.axis_index("patch"), 2)
    here = place(stride, size)
    cut = pieces[0].shape[1]
    for side in range(2):
        base = (core if side == 0 else 1 - core) * (cut * size)
        for k in range(size):
            start = pl.multiple_of(base + (here ^ k) * cut, cut)
            for which, out_ref in enumerate(outputs):
                out_ref[pl.ds(start, cut), :] = pieces[side * size + k][which].astype(F32) * scale


def body(
    grid_latent,
    mesh_latent,
    mesh_cotangent,
    grid_rows,
    mesh_rows,
    counts,
    w1_grid,
    w1_mesh,
    bias_one,
    w2,
):
    members = lax.axis_size("patch")
    slots = grid_rows.shape[0]
    capacity = slots // members
    width = grid_latent.shape[1]
    nodes = mesh_latent.shape[0]
    points = grid_latent.shape[0]
    if capacity != SUB + HALF or members & (members - 1):
        raise ValueError("slot layout")
    scale = 1.0 / math.sqrt(members * slots)
    steps = []
    rest, stride = members // 2, 2
    while rest > 1:
        size = 4 if rest % 4 == 0 else 2
        steps.append((stride, size))
        rest, stride = rest // size, stride * size

    swap = functools.partial(
        lax.all_to_all, axis_name="patch", split_axis=0, concat_axis=0, tiled=True
    )
    wanted = swap(grid_rows.reshape(members, capacity))
    rows2d = mesh_rows.reshape(members, capacity)
    slot = jnp.arange(capacity, dtype=jnp.int32)[None, :]
    live2d = jnp.where(slot < counts[0][:, None], rows2d, -1)
    packed = (members, SUB, width + width // 2)
    count = next(k for k in (8, 4, 2, 1) if points % (k * SUB) == 0)
    found = pl.pallas_call(
        gather_kernel,
        out_shape=pltpu.VMEM(packed, BF16),
        in_specs=[WHOLE, FAR],
        out_specs=WHOLE,
        scratch_shapes=[
            pltpu.VMEM((count, points // count, width), BF16),
            pltpu.SemaphoreType.DMA((count,)),
        ],
        compiler_params=GRANT,
        cost_estimate=pl.CostEstimate(
            flops=2 * slots * points * width, transcendentals=0, bytes_accessed=2 * points * width
        ),
    )(near(wanted), far(grid_latent))
    got = swap(found)
    flat = (slots, width)
    halves = (3, width // 2, width)
    sent, kept, pre = call(
        edge_kernel,
        [(halves, BF16), (halves, F32), (flat, BF16)],
        [
            pltpu.VMEM((3, width, width), F32),
            pltpu.VMEM((nodes, width), BF16),
            pltpu.VMEM((nodes, width), BF16),
            pltpu.SemaphoreType.DMA((2,)),
        ],
        flops=14 * slots * width**2,
        specs=[WHOLE, WHOLE, WHOLE, FAR, FAR, WHOLE, WHOLE, WHOLE, WHOLE],
    )(
        got,
        rows2d,
        live2d,
        mesh_latent,
        mesh_cotangent,
        w1_mesh,
        w2,
        bias_one.reshape(1, width),
        w1_grid,
    )

    came = [send(sent, 1, members)]
    own = kept
    after = None
    for stride, size in steps:
        own, *away = fold(own, came, stride, size)
        came = [send(part, k * stride, members) for k, part in enumerate(away, 1)]
        after = own if after is None else after

    wide = (members, SUB, 2 * width - width // 2 + 128)
    leaving = call(return_kernel, [(wide, BF16)], flops=2 * slots * width**2)(pre, w1_grid, after)[0]
    returned = swap(leaving)
    mesh_grad = call(
        node_kernel, [((nodes, width), F32)], flops=8 * nodes * width**2, leaves=True
    )(rows2d, pre, w1_mesh, after)[0]

    pieces = [fold(own, came, 1, 1)[0]]
    for position, (stride, size) in reversed(list(enumerate(steps))):
        share = pieces[0]
        pieces = [share] + [send(share, k * stride, members) for k in range(1, size)]
        if position > 0:
            pieces = [join(pieces, stride)]
    stride, size = steps[0]
    block = min(512, points)
    grid_grad = pl.pallas_call(
        scatter_kernel,
        out_shape=jax.ShapeDtypeStruct((points, width), F32),
        grid=(points // block,),
        compiler_params=GRANT,
        in_specs=[WHOLE, WHOLE, WHOLE],
        out_specs=pl.BlockSpec((block, width), lambda i: (i, 0)),
        scratch_shapes=[pltpu.VMEM(flat, BF16), pltpu.VMEM((SUB, slots), jnp.int32)],
        cost_estimate=pl.CostEstimate(
            flops=2 * slots * points * width, transcendentals=0, bytes_accessed=4 * points * width
        ),
    )(near(wanted), near(returned), near(pieces[0]))
    others = [send(piece, 1, members) for piece in pieces]
    grads = call(
        functools.partial(final_kernel, scale, stride, size), [((width, width), F32)] * 3, leaves=True
    )(*pieces, *others)
    bias_grad = call(functools.partial(bias_kernel, scale), [((1, width), F32)], leaves=True)(
        returned
    )[0]
    return (grid_grad, mesh_grad, *grads, bias_grad.reshape(width))


def solution(mesh):
    rows, line = P("patch", None), P("patch")
    return jax.shard_map(
        body,
        mesh=mesh,
        in_specs=(rows, rows, rows, line, line, rows, P(), P(), P(), P()),
        out_specs=(rows, rows, P(), P(), P(), P()),
        check_vma=False,
    )
```

```python
import functools
import math

import jax
import jax.numpy as jnp
from jax import lax
from jax.experimental import pallas as pl
from jax.experimental.pallas import tpu as pltpu
from jax.sharding import PartitionSpec as P


SUB = 8
BLOCK = 512
RING = 4
HALF = SUB // 2
F32 = jnp.float32
BF16 = jnp.bfloat16
WHOLE = pl.BlockSpec(memory_space=pltpu.VMEM)
FAR = pl.BlockSpec(memory_space=pltpu.HBM)
GRANT = pltpu.CompilerParams(vmem_limit_bytes=32 << 20)


def dot(left, right, dims=((1,), (0,))):
    return lax.dot_general(left, right, (dims, ((), ())), preferred_element_type=F32)


def near(value):
    return pltpu.with_memory_space_constraint(value, pltpu.VMEM)


def far(value):
    return pltpu.with_memory_space_constraint(value, pltpu.HBM)


def call(kernel, outs, scratch=(), flops=0, leaves=False, specs=None):
    make = jax.ShapeDtypeStruct if leaves else pltpu.VMEM
    built = pl.pallas_call(
        kernel,
        **({} if specs is None else {"in_specs": [spec or WHOLE for spec in specs]}),
        out_shape=[make(shape, dtype) for shape, dtype in outs],
        scratch_shapes=list(scratch),
        compiler_params=GRANT,
        cost_estimate=pl.CostEstimate(flops=flops, transcendentals=0, bytes_accessed=0),
    )

    def run(*values):
        places = [WHOLE] * len(values) if specs is None else specs
        moved = [
            value if spec is None else far(value) if spec is FAR else near(value)
            for spec, value in zip(places, values)
        ]
        return built(*moved)

    return run


def column(index):
    members, capacity = index.shape
    middle = members // 2
    lane = lax.broadcasted_iota(jnp.int32, (members, SUB, capacity), 2)
    row = lax.broadcasted_iota(jnp.int32, (members, SUB, capacity), 1)
    spread = jnp.broadcast_to(index[:, None, :], (members, SUB, capacity))
    head = jnp.sum(jnp.where(lane == row, spread, 0).astype(F32), axis=2, keepdims=True)
    upper = row[:middle] < HALF
    chosen = jnp.where(upper, spread[:middle], spread[middle:])
    wanted = jnp.where(upper, row[:middle] + SUB, row[:middle] + HALF)
    tail = jnp.sum(jnp.where(lane[:middle] == wanted, chosen, 0).astype(F32), axis=2, keepdims=True)
    return jnp.concatenate(
        (head.reshape(members * SUB, 1), tail.reshape(middle * SUB, 1)), axis=0
    ).astype(jnp.int32)


def lanes(index):
    col = column(index).astype(F32)
    return jnp.transpose(jnp.broadcast_to(col, (col.shape[0], 128)))[:1].astype(jnp.int32)


def pick(col, start, size):
    at = lax.broadcasted_iota(jnp.int32, (col.shape[0], size), 1) + start
    return jnp.where(at == col, 1.0, 0.0).astype(BF16)


def pack(rows, members):
    width = rows.shape[1]
    middle = members // 2
    head = rows[: members * SUB].reshape(members, SUB, width)
    tail = rows[members * SUB :].reshape(middle, SUB, width)
    left, right = tail[:, :, : width // 2], tail[:, :, width // 2 :]
    upper = lax.broadcasted_iota(jnp.int32, left.shape, 1) < HALF
    first = jnp.where(upper, left, pltpu.roll(right, HALF, 1))
    second = jnp.where(upper, pltpu.roll(left, HALF, 1), right)
    return head, jnp.concatenate((first, second), axis=0)


def unpack(packed, width):
    members = packed.shape[0]
    middle = members // 2
    head = packed[:, :, :width].reshape(members * SUB, width)
    first = packed[:middle, :, width : width + width // 2]
    second = packed[middle:, :, width : width + width // 2]
    upper = lax.broadcasted_iota(jnp.int32, first.shape, 1) < HALF
    left = jnp.where(upper, first, pltpu.roll(second, HALF, 1))
    right = jnp.where(upper, pltpu.roll(first, HALF, 1), second)
    tail = jnp.concatenate((left, right), axis=2).reshape(middle * SUB, width)
    return jnp.concatenate((head, tail), axis=0)


def gather_kernel(index_ref, table_ref, out_ref, held_ref, sems):
    members = index_ref.shape[0]
    width = table_ref.shape[1]
    count, step, _ = held_ref.shape
    copies = [
        pltpu.make_async_copy(table_ref.at[pl.ds(k * step, step), :], held_ref.at[k], sems.at[k])
        for k in range(count)
    ]
    for copy in copies:
        copy.start()
    col = column(index_ref[...])
    total = None
    for k, copy in enumerate(copies):
        chosen = pick(col, k * step, step)
        copy.wait()
        part = dot(chosen, held_ref[k])
        total = part if total is None else total + part
    head, tail = pack(total, members)
    out_ref[:, :, :width] = head.astype(BF16)
    out_ref[:, :, width:] = tail.astype(BF16)


def mesh_kernel(
    rows_ref, live_ref, latent_ref, cot_ref, w1_ref, w2_ref, bias_ref, in_ref, grad_ref, base_ref, hid_ref
):
    nodes = latent_ref.shape[0]
    mesh_in = dot(pick(column(rows_ref[...]), 0, nodes), latent_ref[...]).astype(BF16)
    out_grad = dot(pick(column(live_ref[...]), 0, nodes), cot_ref[...]).astype(BF16)
    in_ref[...] = mesh_in
    grad_ref[...] = out_grad
    base_ref[...] = dot(mesh_in, w1_ref[...]) + bias_ref[...]
    hid_ref[...] = dot(out_grad, w2_ref[...], ((1,), (1,)))


def edge_kernel(
    got_ref,
    base_hbm,
    hid_hbm,
    mesh_hbm,
    grad_hbm,
    w1_ref,
    sent_ref,
    kept_ref,
    pre_ref,
    full_ref,
    base_ref,
    hid_ref,
    mesh_ref,
    grad_ref,
    sems,
):
    loads = [
        pltpu.make_async_copy(source, held, sems.at[which])
        for which, (source, held) in enumerate(
            ((base_hbm, base_ref), (hid_hbm, hid_ref), (mesh_hbm, mesh_ref), (grad_hbm, grad_ref))
        )
    ]
    for load in loads:
        load.start()
    width = mesh_ref.shape[1]
    half = sent_ref.shape[1]
    core = lax.rem(lax.axis_index("patch"), 2)
    grid_in = unpack(got_ref[...].astype(F32), width).astype(BF16)
    grid_proj = dot(grid_in, w1_ref[...]).astype(BF16).astype(F32)
    loads[0].wait()
    before = grid_proj + base_ref[...]
    logistic = jax.nn.sigmoid(before)
    hidden = (before * logistic).astype(BF16)
    derivative = logistic * (1.0 + before * (1.0 - logistic))
    loads[1].wait()
    pre = (hid_ref[...] * derivative).astype(BF16)
    pre_ref[...] = pre
    across = ((0,), (0,))
    full_ref[0] = dot(grid_in, pre, across)
    loads[2].wait()
    full_ref[1] = dot(mesh_ref[...], pre, across)
    loads[3].wait()
    full_ref[2] = dot(hidden, grad_ref[...], across)
    away = pl.multiple_of((1 - core) * half, half)
    home = pl.multiple_of(core * half, half)
    for which in range(3):
        sent_ref[which] = full_ref[which, pl.ds(away, half), :].astype(BF16)
        kept_ref[which] = full_ref[which, pl.ds(home, half), :]


def return_kernel(pre_ref, w1_ref, out_ref):
    members = out_ref.shape[0]
    width = pre_ref.shape[1]
    pre = pre_ref[...]
    head, tail = pack(dot(pre, w1_ref[...], ((1,), (1,))), members)
    out_ref[:, :, :width] = head.astype(BF16)
    out_ref[:, :, width : width + width // 2] = tail.astype(BF16)
    bias = jnp.sum(pre.astype(F32), axis=0, keepdims=True)
    high = bias.astype(BF16).astype(F32)
    low = bias - high
    at = lax.broadcasted_iota(jnp.int32, (SUB, 128), 0)
    tile = jnp.zeros((SUB, 128), F32)
    for part in range(width // 128):
        block = slice(part * 128, part * 128 + 128)
        tile = jnp.where(at == part, high[:, block], tile)
        tile = jnp.where(at == part + width // 128, low[:, block], tile)
    out_ref[:, :, width + width // 2 :] = jnp.broadcast_to(tile[None], (members, SUB, 128)).astype(
        BF16
    )


def scatter_kernel(
    scale, index_ref, came_ref, after_ref, out_ref, bias_ref, rows_ref, held_ref, sems
):
    ring, size, width = held_ref.shape
    rows_ref[...] = unpack(came_ref[...].astype(F32), width).astype(BF16)
    flat = lanes(index_ref[...])
    copies = []
    for step in range(out_ref.shape[0] // size):
        slot = step % ring
        if step >= ring:
            copies[step - ring].wait()
        at = lax.broadcasted_iota(jnp.int32, (size, rows_ref.shape[0]), 0) + step * size
        chosen = jnp.where(at == flat, 1.0, 0.0).astype(BF16)
        held_ref[slot] = dot(chosen, rows_ref[...])
        copy = pltpu.make_async_copy(
            held_ref.at[slot], out_ref.at[pl.ds(step * size, size), :], sems.at[slot]
        )
        copy.start()
        copies.append(copy)
    tile = jnp.sum(came_ref[:, :, width + width // 2 :].astype(F32), axis=0)
    for part in range(width // 128):
        low = part + width // 128
        bias_ref[:, part * 128 : part * 128 + 128] = (
            tile[part : part + 1] + tile[low : low + 1]
        ) * scale
    for copy in copies[-ring:]:
        copy.wait()


def node_kernel(rows_ref, pre_ref, w1_ref, after_ref, out_ref):
    nodes = out_ref.shape[0]
    flat = lanes(rows_ref[...])
    at = lax.broadcasted_iota(jnp.int32, (nodes, flat.shape[1]), 0)
    sums = dot(jnp.where(at == flat, 1.0, 0.0).astype(BF16), pre_ref[...])
    total = None
    for _ in range(3):
        piece = sums.astype(BF16)
        part = dot(piece, w1_ref[...], ((1,), (1,)))
        total = part if total is None else total + part
        sums = sums - piece.astype(F32)
    out_ref[...] = total


def place(stride, size):
    return lax.rem(lax.div(lax.axis_index("patch"), stride), size)


def fold(own, came, stride, size):
    count, rows, width = own.shape
    cut = rows // size

    def kernel(*refs):
        inputs, outputs = refs[: 1 + len(came)], refs[1 + len(came) :]
        here = place(stride, size) if size > 1 else 0
        for k, out_ref in enumerate(outputs):
            start = pl.multiple_of((here ^ k) * cut, cut) if size > 1 else 0
            total = sum(ref[:, pl.ds(start, cut), :].astype(F32) for ref in inputs)
            out_ref[...] = total.astype(out_ref.dtype)

    types = [F32 if k == 0 and size > 1 else BF16 for k in range(size)]
    if cut % 16 == 0:
        return call(kernel, [((count, cut, width), dtype) for dtype in types])(own, *came)
    total = own.astype(F32) + sum(part.astype(F32) for part in came)
    here = place(stride, size) if size > 1 else 0
    return [
        lax.dynamic_slice_in_dim(total, (here ^ k) * cut, cut, axis=1).astype(dtype)
        for k, dtype in enumerate(types)
    ]


def join(pieces, stride):
    count, cut, width = pieces[0].shape
    size = len(pieces)

    def kernel(*refs):
        here = place(stride, size)
        for k in range(size):
            start = pl.multiple_of((here ^ k) * cut, cut)
            refs[-1][:, pl.ds(start, cut), :] = refs[k][...]

    if cut % 16 == 0:
        return call(kernel, [((count, cut * size, width), BF16)])(*pieces)[0]
    order = jnp.arange(size, dtype=jnp.int32) ^ place(stride, size)
    return jnp.take(jnp.stack(pieces, axis=1), order, axis=1).reshape(count, cut * size, width)


def send(value, step, members):
    return lax.ppermute(value, "patch", [(i, i ^ step) for i in range(members)])


def final_kernel(scale, stride, size, *refs):
    pieces = refs[: 2 * size]
    *outputs, held_ref, sems = refs[2 * size :]
    core = lax.rem(lax.axis_index("patch"), 2)
    here = place(stride, size)
    cut = pieces[0].shape[1]
    copies = []
    for which, out_ref in enumerate(outputs):
        for side in range(2):
            base = (core if side == 0 else 1 - core) * (cut * size)
            for k in range(size):
                start = pl.multiple_of(base + (here ^ k) * cut, cut)
                held_ref[which, pl.ds(start, cut), :] = (
                    pieces[side * size + k][which].astype(F32) * scale
                )
        copy = pltpu.make_async_copy(held_ref.at[which], out_ref, sems.at[which])
        copy.start()
        copies.append(copy)
    for copy in copies:
        copy.wait()


def body(
    grid_latent,
    mesh_latent,
    mesh_cotangent,
    grid_rows,
    mesh_rows,
    counts,
    w1_grid,
    w1_mesh,
    bias_one,
    w2,
):
    members = lax.axis_size("patch")
    slots = grid_rows.shape[0]
    capacity = slots // members
    width = grid_latent.shape[1]
    nodes = mesh_latent.shape[0]
    points = grid_latent.shape[0]
    if capacity != SUB + HALF or members & (members - 1):
        raise ValueError("slot layout")
    scale = 1.0 / math.sqrt(members * slots)
    steps = []
    rest, stride = members // 2, 2
    while rest > 1:
        size = 4 if rest % 4 == 0 else 2
        steps.append((stride, size))
        rest, stride = rest // size, stride * size

    swap = functools.partial(
        lax.all_to_all, axis_name="patch", split_axis=0, concat_axis=0, tiled=True
    )
    wanted = swap(grid_rows.reshape(members, capacity))
    rows2d = mesh_rows.reshape(members, capacity)
    slot = jnp.arange(capacity, dtype=jnp.int32)[None, :]
    live2d = jnp.where(slot < counts[0][:, None], rows2d, -1)
    packed = (members, SUB, width + width // 2)
    count = next(k for k in (8, 4, 2, 1) if points % (k * SUB) == 0)
    found = pl.pallas_call(
        gather_kernel,
        out_shape=pltpu.VMEM(packed, BF16),
        in_specs=[WHOLE, FAR],
        out_specs=WHOLE,
        scratch_shapes=[
            pltpu.VMEM((count, points // count, width), BF16),
            pltpu.SemaphoreType.DMA((count,)),
        ],
        compiler_params=GRANT,
        cost_estimate=pl.CostEstimate(
            flops=2 * slots * points * width, transcendentals=0, bytes_accessed=2 * points * width
        ),
    )(near(wanted), far(grid_latent))
    got = swap(found)
    flat = (slots, width)
    halves = (3, width // 2, width)
    mesh_side = [(flat, BF16), (flat, BF16), (flat, F32), (flat, F32)]
    mesh_in, out_grad, base, hid = call(
        mesh_kernel, mesh_side, flops=8 * slots * width**2, leaves=True, specs=[WHOLE] * 2 + [None] * 5
    )(rows2d, live2d, mesh_latent, mesh_cotangent, w1_mesh, w2, bias_one.reshape(1, width))
    sent, kept, pre = call(
        edge_kernel,
        [(halves, BF16), (halves, F32), (flat, BF16)],
        [
            pltpu.VMEM((3, width, width), F32),
            pltpu.VMEM(flat, F32),
            pltpu.VMEM(flat, F32),
            pltpu.VMEM(flat, BF16),
            pltpu.VMEM(flat, BF16),
            pltpu.SemaphoreType.DMA((4,)),
        ],
        flops=8 * slots * width**2,
        specs=[WHOLE, FAR, FAR, FAR, FAR, WHOLE],
    )(got, base, hid, mesh_in, out_grad, w1_grid)

    came = [send(sent, 1, members)]
    own = kept
    after = None
    for stride, size in steps:
        own, *away = fold(own, came, stride, size)
        came = [send(part, k * stride, members) for k, part in enumerate(away, 1)]
        after = own if after is None else after

    wide = (members, SUB, 2 * width - width // 2 + 128)
    leaving = call(return_kernel, [(wide, BF16)], flops=2 * slots * width**2)(pre, w1_grid)[0]
    returned = swap(leaving)
    mesh_grad = call(
        node_kernel, [((nodes, width), F32)], flops=8 * nodes * width**2, leaves=True
    )(rows2d, pre, w1_mesh, after)[0]

    pieces = [fold(own, came, 1, 1)[0]]
    for position, (stride, size) in reversed(list(enumerate(steps))):
        share = pieces[0]
        pieces = [share] + [send(share, k * stride, members) for k in range(1, size)]
        if position > 0:
            pieces = [join(pieces, stride)]
    stride, size = steps[0]
    block = min(BLOCK, points)
    ring = min(RING, points // block)
    grid_grad, bias_grad = pl.pallas_call(
        functools.partial(scatter_kernel, scale),
        out_shape=[
            jax.ShapeDtypeStruct((points, width), F32),
            jax.ShapeDtypeStruct((1, width), F32),
        ],
        compiler_params=GRANT,
        in_specs=[WHOLE, WHOLE, WHOLE],
        out_specs=[FAR, WHOLE],
        scratch_shapes=[
            pltpu.VMEM(flat, BF16),
            pltpu.VMEM((ring, block, width), F32),
            pltpu.SemaphoreType.DMA((ring,)),
        ],
        cost_estimate=pl.CostEstimate(
            flops=2 * slots * points * width, transcendentals=0, bytes_accessed=4 * points * width
        ),
    )(near(wanted), near(returned), near(pieces[0]))
    others = [send(piece, 1, members) for piece in pieces]
    grads = pl.pallas_call(
        functools.partial(final_kernel, scale, stride, size),
        out_shape=[jax.ShapeDtypeStruct((width, width), F32)] * 3,
        out_specs=[FAR] * 3,
        scratch_shapes=[pltpu.VMEM((3, width, width), F32), pltpu.SemaphoreType.DMA((3,))],
        compiler_params=GRANT,
    )(*map(near, (*pieces, *others)))
    return (grid_grad, mesh_grad, *grads, bias_grad.reshape(width))


def solution(mesh):
    rows, line = P("patch", None), P("patch")
    return jax.shard_map(
        body,
        mesh=mesh,
        in_specs=(rows, rows, rows, line, line, rows, P(), P(), P(), P()),
        out_specs=(rows, rows, P(), P(), P(), P()),
        check_vma=False,
    )
```
